32 devices in a mesh: dp: 1 (over z), tp: 4 (over y), cp: 8 (over x, core).
Axes of the slice: x: 4, y: 4, z: 1, core: 2. Of those that a mesh axis runs over, the one named last changes fastest.
The devices are a block of a 4x4x8 slice.
Arguments:
- hidden: bfloat16 [2048, 6144], P(('dp', 'cp'))
- seg_ids: int32 [2048], P(('dp', 'cp'))
- w_q: bfloat16 [6144, 6144], P(None, 'tp')
- b_q: bfloat16 [6144], P('tp')
- w_kv: bfloat16 [6144, 256], replicated
- b_kv: bfloat16 [256], replicated
- w_o: bfloat16 [6144, 6144], P('tp')
- b_o: bfloat16 [6144], replicated
- ln_gain: bfloat16 [6144], replicated
- ln_bias: bfloat16 [6144], replicated
Outputs:
- output 1: bfloat16 [2048, 6144], P(('dp', 'cp'))
- output 2: bfloat16 [2048, 128], P(('dp', 'cp'))
- output 3: bfloat16 [2048, 128], P(('dp', 'cp'))
All inputs are finite; a program needn't handle non-finite values.
Results may differ from the reference program's by a relative error of at most 0.0128034.
Values are sent between devices in bfloat16 or wider.
A program may use at most 768 MiB of HBM per device.

```python
import jax
import jax.numpy as jnp
from jax import lax

D_MODEL = 6144
N_HEADS = 48
HEAD_DIM = 128
TOKENS = 2048
HEAD_GROUPS = 4

LN_EPS = 1e-5
ATTN_SCALE = HEAD_DIM ** -0.5
QUERY_ROWS = min(TOKENS, 64)


def draw_segments(seg_key):
    len_low = TOKENS // 27 + 1
    len_high = (TOKENS * 5) // 8
    max_prompts = TOKENS // len_low + 1
    lengths = jax.random.randint(seg_key, (max_prompts,), len_low, len_high + 1, dtype=jnp.int32)
    prompt_ends = jnp.cumsum(lengths)
    positions = jnp.arange(TOKENS, dtype=jnp.int32)
    return jnp.sum((positions[:, None] >= prompt_ends[None, :]).astype(jnp.int32), axis=1)


def setup_inputs(seed: int = 0, part: int = 0) -> dict:
    part_key = jax.random.fold_in(jax.random.key(seed), part)
    key_hidden, key_seg = jax.random.split(part_key)
    shared = jax.random.split(jax.random.key(seed + 1), 8)
    q_width = N_HEADS * HEAD_DIM
    hidden = (0.5 * jax.random.normal(key_hidden, (TOKENS, D_MODEL), jnp.float32)).astype(jnp.bfloat16)
    seg_ids = draw_segments(key_seg)
    w_q = (1.6 * D_MODEL ** -0.5 * jax.random.normal(shared[0], (D_MODEL, q_width), jnp.float32)).astype(jnp.bfloat16)
    b_q = (0.3 * jax.random.normal(shared[1], (q_width,), jnp.float32)).astype(jnp.bfloat16)
    w_kv = (1.6 * D_MODEL ** -0.5 * jax.random.normal(shared[2], (D_MODEL, 2 * HEAD_DIM), jnp.float32)).astype(jnp.bfloat16)
    b_kv = (0.2 * jax.random.normal(shared[3], (2 * HEAD_DIM,), jnp.float32)).astype(jnp.bfloat16)
    w_o = (q_width ** -0.5 * jax.random.normal(shared[4], (q_width, D_MODEL), jnp.float32)).astype(jnp.bfloat16)
    b_o = (0.3 * jax.random.normal(shared[5], (D_MODEL,), jnp.float32)).astype(jnp.bfloat16)
    ln_gain = (1.0 + 0.3 * jax.random.normal(shared[6], (D_MODEL,), jnp.float32)).astype(jnp.bfloat16)
    ln_bias = (0.3 * jax.random.normal(shared[7], (D_MODEL,), jnp.float32)).astype(jnp.bfloat16)
    return dict(hidden=hidden, seg_ids=seg_ids, w_q=w_q, b_q=b_q, w_kv=w_kv, b_kv=b_kv, w_o=w_o, b_o=b_o, ln_gain=ln_gain, ln_bias=ln_bias)


def reference(hidden, seg_ids, w_q, b_q, w_kv, b_kv, w_o, b_o, ln_gain, ln_bias):
    x_float = hidden.astype(jnp.float32)
    centered = x_float - jnp.mean(x_float, axis=-1, keepdims=True)
    variance = jnp.mean(centered * centered, axis=-1, keepdims=True)
    normed = (centered * lax.rsqrt(variance + LN_EPS) * ln_gain.astype(jnp.float32) + ln_bias.astype(jnp.float32)).astype(jnp.bfloat16)
    q_all = (jnp.dot(normed, w_q, preferred_element_type=jnp.float32) + b_q.astype(jnp.float32)).astype(jnp.bfloat16)
    kv_all = (jnp.dot(normed, w_kv, preferred_element_type=jnp.float32) + b_kv.astype(jnp.float32)).astype(jnp.bfloat16)
    k_cache = kv_all[:, :HEAD_DIM]
    v_cache = kv_all[:, HEAD_DIM:]
    k_float = k_cache.astype(jnp.float32)
    v_float = v_cache.astype(jnp.float32)
    positions = jnp.arange(TOKENS, dtype=jnp.int32)
    n_blocks = TOKENS // QUERY_ROWS
    q_blocks = q_all.reshape(n_blocks, QUERY_ROWS, N_HEADS, HEAD_DIM)
    seg_blocks = seg_ids.reshape(n_blocks, QUERY_ROWS)
    pos_blocks = positions.reshape(n_blocks, QUERY_ROWS)

    def attend(block_in):
        q_blk, seg_q, pos_q = block_in
        scores = jnp.einsum('bhd,kd->bhk', q_blk.astype(jnp.float32), k_float) * ATTN_SCALE
        visible = (seg_ids[None, :] == seg_q[:, None]) & (positions[None, :] <= pos_q[:, None])
        scores = jnp.where(visible[:, None, :], scores, -jnp.inf)
        p_weights = jax.nn.softmax(scores, axis=-1)
        return jnp.einsum('bhk,kd->bhd', p_weights, v_float).astype(jnp.bfloat16)

    attn_out = lax.map(attend, (q_blocks, seg_blocks, pos_blocks))
    group_width = N_HEADS * HEAD_DIM // HEAD_GROUPS
    attn_groups = attn_out.reshape(TOKENS, HEAD_GROUPS, group_width).transpose(1, 0, 2)
    wo_groups = w_o.reshape(HEAD_GROUPS, group_width, D_MODEL)

    def add_group(run_total, group_pair):
        attn_g, wo_g = group_pair
        partial = jnp.dot(attn_g, wo_g, preferred_element_type=jnp.float32).astype(jnp.bfloat16)
        return run_total + partial.astype(jnp.float32), None

    proj_sum, scan_tail = lax.scan(add_group, jnp.zeros((TOKENS, D_MODEL), jnp.float32), (attn_groups, wo_groups))
    y_out = (x_float + proj_sum + b_o.astype(jnp.float32)).astype(jnp.bfloat16)
    return (y_out, k_cache, v_cache)
```

```python
import functools

import jax
import jax.numpy as jnp
from jax import lax
from jax.experimental import pallas as pl
from jax.experimental.pallas import tpu as pltpu
from jax.sharding import PartitionSpec as P

HEAD_DIM = 128
LN_EPS = 1e-5
SCORE_EXP2 = HEAD_DIM ** -0.5 * 1.4426950408889634
PIECE = 64
SEG_ROWS = 16
MESH_ID = pl.DeviceIdType.MESH
F32 = jnp.float32
BF16 = jnp.bfloat16


def each(lo, hi, body):
    def step(i, carry):
        body(i)
        return carry
    lax.fori_loop(lo, hi, step, 0)


def block_kernel(n_tp, n_cp, hid_hbm, seg_ref, wq_hbm, bq_ref, wkv_hbm, bkv_ref, wo_hbm, bo_ref, gain_ref, lnb_ref,
                 y_hbm, k_ref, v_ref,
                 hid, normed, gain_b, bias_b, wkv, wq, wo, kvbuf, segq, q_s, m_s, l_s, acc_s, o_s, stage, recv, y_v,
                 hid_sem, wkv_sem, wq_sem, wo_sem, kv_send, fwd_send, kv_recv, msg_send, msg_recv,
                 ag_send, ag_recv, fw_send, fw_recv, out_sem):
    tok, d_model = hid.shape
    n_heads = q_s.shape[1] // PIECE
    n_piece = tok // PIECE
    n_chip = n_cp // 2
    chunk = d_model // n_tp
    half = chunk // 2
    me_t = lax.axis_index('tp')
    me_c = lax.axis_index('cp')
    chip = me_c // 2
    core = me_c % 2
    sibling = me_c + 1 - 2 * core
    right = (me_t + 1) % n_tp
    left = (me_t + n_tp - 1) % n_tp
    across = (me_t + 2) % n_tp

    ln_rows = tok // 4
    def load_hid(i):
        rows = pl.ds(i * ln_rows, ln_rows)
        return pltpu.make_async_copy(hid_hbm.at[rows, :], hid.at[rows, :], hid_sem.at[i])
    def load_wkv():
        return pltpu.make_async_copy(wkv_hbm, wkv, wkv_sem)
    def load_wq(i):
        return pltpu.make_async_copy(wq_hbm.at[:, pl.ds(i * 256, 256)], wq.at[i], wq_sem.at[i])
    slots = ((across, 0), (across, 1), (right, 1), (left, 0), (right, 0), (left, 1), (me_t, 0), (me_t, 1))
    def load_wo(i):
        owner, part = slots[i]
        cols = pl.ds(pl.multiple_of(owner * chunk + part * half, 128), half)
        return pltpu.make_async_copy(wo_hbm.at[:, cols], wo.at[i], wo_sem.at[i])
    for i in range(4):
        load_hid(i).start()
    load_wkv().start()
    for i in range(wq.shape[0]):
        load_wq(i).start()
    for i in range(8):
        load_wo(i).start()

    barrier = pltpu.get_barrier_semaphore()
    peers = [{'tp': left}, {'tp': right}, {'cp': sibling}] + [{'cp': (me_c + 2 * d) % n_cp} for d in range(1, n_chip)]
    for peer in peers:
        pl.semaphore_signal(barrier, inc=1, device_id=peer, device_id_type=MESH_ID)

    gain_b[...] = jnp.broadcast_to(gain_ref[...].astype(F32), gain_b.shape)
    bias_b[...] = jnp.broadcast_to(lnb_ref[...].astype(F32), bias_b.shape)
    for i in range(4):
        load_hid(i).wait()
        def norm_rows(r, i=i):
            rows = pl.ds(pl.multiple_of(i * ln_rows + r * 16, 16), 16)
            x = hid[rows, :].astype(F32)
            centered = x - jnp.mean(x, axis=-1, keepdims=True)
            variance = jnp.mean(centered * centered, axis=-1, keepdims=True)
            normed[rows, :] = (centered * lax.rsqrt(variance + LN_EPS) * gain_b[...] + bias_b[...]).astype(BF16)
        each(0, ln_rows // 16, norm_rows)

    seg = seg_ref[...]
    seg_high = (seg // 256).astype(F32)
    seg_low = (seg % 256).astype(F32)
    row_id = lax.broadcasted_iota(jnp.int32, (SEG_ROWS, tok), 0)
    kvbuf[me_c, tok:, :] = jnp.where(row_id == 0, seg_high, jnp.where(row_id == 1, seg_low, 0.0)).astype(BF16)
    seg_f = seg.astype(F32)
    for b in range(tok // 128):
        column = jnp.broadcast_to(seg_f[:, b * 128:(b + 1) * 128], (128, 128)).T
        for s in range(128 // PIECE):
            part = column[s * PIECE:(s + 1) * PIECE]
            segq[b * (128 // PIECE) + s] = jnp.concatenate([part] * (tok // 128), axis=1)

    load_wkv().wait()
    kv = (jnp.dot(normed[...], wkv[...], preferred_element_type=F32) + bkv_ref[...].astype(F32)).astype(BF16)
    kvbuf[me_c, :tok, :] = kv
    k_ref[...] = kv[:, :HEAD_DIM]
    v_ref[...] = kv[:, HEAD_DIM:]
    pl.semaphore_wait(barrier, len(peers))

    def send_kv(block, target, send_sem):
        return pltpu.make_async_remote_copy(src_ref=kvbuf.at[block], dst_ref=kvbuf.at[block], send_sem=send_sem,
                                            recv_sem=kv_recv.at[block], device_id={'cp': target}, device_id_type=MESH_ID)
    for d in range(n_chip - 1, 0, -1):
        @pl.when(chip + d < n_chip)
        def _(d=d):
            send_kv(me_c, (me_c + 2 * d) % n_cp, kv_send.at[d]).start()
    @pl.when(core == 0)
    def _():
        send_kv(me_c, sibling, kv_send.at[0]).start()

    for i in range(wq.shape[0]):
        load_wq(i).wait()
        q = (jnp.dot(normed[...], wq[i], preferred_element_type=F32) + bq_ref[:, i * 256:(i + 1) * 256].astype(F32)).astype(BF16)
        for piece in range(n_piece):
            for h in range(2):
                q_s[piece, (2 * i + h) * PIECE:(2 * i + h + 1) * PIECE, :] = q[piece * PIECE:(piece + 1) * PIECE, h * HEAD_DIM:(h + 1) * HEAD_DIM]

    def attend(piece, block, first):
        q = q_s[piece]
        k_blk = kvbuf[block, :tok, :HEAD_DIM]
        v_blk = kvbuf[block, :tok, HEAD_DIM:]
        digits = kvbuf[block, tok:, :].astype(F32)
        seg_key = digits[0:1] * 256.0 + digits[1:2]
        visible = segq[piece] == seg_key
        if first:
            q_pos = lax.broadcasted_iota(jnp.int32, (PIECE, tok), 0) + piece * PIECE
            visible = visible & (lax.broadcasted_iota(jnp.int32, (PIECE, tok), 1) <= q_pos)
        s = lax.dot_general(q, k_blk, (((1,), (1,)), ((), ())), preferred_element_type=F32)
        s = jnp.where(visible[None], s.reshape(n_heads, PIECE, tok), -jnp.inf).reshape(n_heads * PIECE, tok)
        m_new = jnp.broadcast_to(jnp.max(s, axis=-1, keepdims=True), (n_heads * PIECE, HEAD_DIM))
        if not first:
            m_prev = m_s[piece]
            m_new = jnp.maximum(m_prev, m_new)
        weights = jnp.exp2((s - jnp.concatenate([m_new] * (tok // HEAD_DIM), axis=1)) * SCORE_EXP2)
        total = jnp.broadcast_to(jnp.sum(weights, axis=-1, keepdims=True), (n_heads * PIECE, HEAD_DIM))
        out = jnp.dot(weights.astype(BF16), v_blk, preferred_element_type=F32)
        m_s[piece] = m_new
        if first:
            l_s[piece] = total
            acc_s[piece] = out
        else:
            rescale = jnp.exp2((m_prev - m_new) * SCORE_EXP2)
            l_s[piece] = l_s[piece] * rescale + total
            acc_s[piece] = acc_s[piece] * rescale + out

    each(0, n_piece, lambda piece: attend(piece, me_c, True))
    @pl.when(core == 1)
    def _():
        send_kv(sibling, sibling, kv_send.at[0]).wait_recv()
        each(0, n_piece, lambda piece: attend(piece, sibling, False))

    def take_far(i):
        same = me_c - 2 * (i + 1)
        other = sibling - 2 * (i + 1)
        passing = send_kv(same, sibling, fwd_send.at[i])
        passing.wait_recv()
        passing.start()
        attend(0, same, False)
        send_kv(other, sibling, fwd_send.at[i]).wait_recv()
        attend(0, other, False)
    each(0, chip, take_far)

    def message(piece, i):
        target = (me_t + 1 + (i % 2) * (n_tp - 2)) % n_tp
        return pltpu.make_async_remote_copy(src_ref=stage.at[piece, i], dst_ref=recv.at[piece, i], send_sem=msg_send.at[piece, i],
                                            recv_sem=msg_recv.at[piece, i], device_id={'tp': target}, device_id_type=MESH_ID)
    def y_part(piece, owner, part):
        return y_v.at[pl.ds(pl.multiple_of(piece * PIECE, PIECE), PIECE), pl.ds(pl.multiple_of(owner * chunk + part * half, 128), half)]
    def gather(piece, way, part):
        ref = y_part(piece, me_t, part)
        return pltpu.make_async_remote_copy(src_ref=ref, dst_ref=ref, send_sem=ag_send.at[piece, way, part],
                                            recv_sem=ag_recv.at[piece, way, part], device_id={'tp': (right, left)[way]}, device_id_type=MESH_ID)
    def pass_on(piece, way):
        ref = y_part(piece, (left, right)[way], way)
        return pltpu.make_async_remote_copy(src_ref=ref, dst_ref=ref, send_sem=fw_send.at[piece, way],
                                            recv_sem=fw_recv.at[piece, way], device_id={'tp': (right, left)[way]}, device_id_type=MESH_ID)
    def put_out(piece):
        rows = pl.ds(pl.multiple_of(piece * PIECE, PIECE), PIECE)
        return pltpu.make_async_copy(y_v.at[rows, :], y_hbm.at[rows, :], out_sem.at[piece])

    for i in range(8):
        load_wo(i).wait()

    def step(s):
        @pl.when(s < n_piece)
        def _():
            @pl.when(s > 0)
            def _():
                each(0, 2 * chip, lambda block: attend(s, block, False))
            attn = (acc_s[s] / l_s[s]).astype(BF16)
            for h in range(n_heads):
                o_s[:, h * HEAD_DIM:(h + 1) * HEAD_DIM] = attn[h * PIECE:(h + 1) * PIECE]
            def project(i):
                stage[s, i] = jnp.dot(o_s[...], wo[i], preferred_element_type=F32).astype(BF16)
                @pl.when(i < 4)
                def _():
                    message(s, i).start()
            each(0, 8, project)
            for i in range(2):
                message(s, i).wait_recv()
                stage[s, 4 + i] = (stage[s, 4 + i].astype(F32) + recv[s, i].astype(F32)).astype(BF16)
                message(s, 4 + i).start()

        @pl.when((s >= 1) & (s < n_piece + 1))
        def _():
            piece = s - 1
            for i in range(2, 6):
                message(piece, i).wait_recv()
            rows = pl.ds(pl.multiple_of(piece * PIECE, PIECE), PIECE)
            for part in range(2):
                cols = pl.ds(pl.multiple_of(me_t * chunk + part * half, 128), half)
                from_left, from_right = ((4, 3), (2, 5))[part]
                proj = stage[piece, 6 + part].astype(F32) + recv[piece, from_left].astype(F32) + recv[piece, from_right].astype(F32)
                y_v[rows, cols] = (hid[rows, cols].astype(F32) + proj + bo_ref[:, cols].astype(F32)).astype(BF16)
                for way in range(2):
                    gather(piece, way, part).start()

        @pl.when((s >= 2) & (s < n_piece + 2))
        def _():
            piece = s - 2
            for way in range(2):
                gather(piece, way, way).wait_recv()
                pass_on(piece, way).start()

        @pl.when(s >= 3)
        def _():
            piece = s - 3
            for way in range(2):
                gather(piece, way, 1 - way).wait_recv()
                pass_on(piece, way).wait_recv()
            put_out(piece).start()
    each(0, n_piece + 3, step)

    def finish(piece):
        for i in range(6):
            message(piece, i).wait_send()
        for way in range(2):
            for part in range(2):
                gather(piece, way, part).wait_send()
            pass_on(piece, way).wait_send()
        put_out(piece).wait()
    each(0, n_piece, finish)
    for d in range(n_chip - 1, 0, -1):
        @pl.when(chip + d < n_chip)
        def _(d=d):
            send_kv(me_c, (me_c + 2 * d) % n_cp, kv_send.at[d]).wait_send()
    @pl.when(core == 0)
    def _():
        send_kv(me_c, sibling, kv_send.at[0]).wait_send()
    each(0, chip, lambda i: send_kv(me_c - 2 * (i + 1), sibling, fwd_send.at[i]).wait_send())


def solution(mesh):
    n_tp, n_cp = mesh.shape['tp'], mesh.shape['cp']

    def local_block(hidden, seg_ids, w_q, b_q, w_kv, b_kv, w_o, b_o, ln_gain, ln_bias):
        tok, d_model = hidden.shape
        width = w_q.shape[1]
        n_piece = tok // PIECE
        n_heads = width // HEAD_DIM
        rows = n_heads * PIECE
        half = d_model // n_tp // 2
        hbm = pl.BlockSpec(memory_space=pl.ANY)
        vmem = pl.BlockSpec(memory_space=pltpu.VMEM)
        dma = pltpu.SemaphoreType.DMA
        scratch = [
            pltpu.VMEM((tok, d_model), BF16),
            pltpu.VMEM((tok, d_model), BF16),
            pltpu.VMEM((16, d_model), F32),
            pltpu.VMEM((16, d_model), F32),
            pltpu.VMEM((d_model, 2 * HEAD_DIM), BF16),
            pltpu.VMEM((width // 256, d_model, 256), BF16),
            pltpu.VMEM((2 * n_tp, width, half), BF16),
            pltpu.VMEM((n_cp, tok + SEG_ROWS, 2 * HEAD_DIM), BF16),
            pltpu.VMEM((n_piece, PIECE, tok), F32),
            pltpu.VMEM((n_piece, rows, HEAD_DIM), BF16),
            pltpu.VMEM((n_piece, rows, HEAD_DIM), F32),
            pltpu.VMEM((n_piece, rows, HEAD_DIM), F32),
            pltpu.VMEM((n_piece, rows, HEAD_DIM), F32),
            pltpu.VMEM((PIECE, width), BF16),
            pltpu.VMEM((n_piece, 8, PIECE, half), BF16),
            pltpu.VMEM((n_piece, 6, PIECE, half), BF16),
            pltpu.VMEM((tok, d_model), BF16),
            dma((4,)), dma, dma((width // 256,)), dma((8,)),
            dma((n_cp // 2,)), dma((n_cp // 2,)), dma((n_cp,)), dma((n_piece, 6)), dma((n_piece, 6)),
            dma((n_piece, 2, 2)), dma((n_piece, 2, 2)), dma((n_piece, 2)), dma((n_piece, 2)), dma((n_piece,)),
        ]
        row = lambda a: a.reshape(1, a.shape[0])
        return pl.pallas_call(
            functools.partial(block_kernel, n_tp, n_cp),
            out_shape=(jax.ShapeDtypeStruct((tok, d_model), BF16), jax.ShapeDtypeStruct((tok, HEAD_DIM), BF16),
                       jax.ShapeDtypeStruct((tok, HEAD_DIM), BF16)),
            in_specs=[hbm, vmem, hbm, vmem, hbm, vmem, hbm, vmem, vmem, vmem],
            out_specs=(hbm, vmem, vmem),
            scratch_shapes=scratch,
            compiler_params=pltpu.CompilerParams(collective_id=0, has_side_effects=True, vmem_limit_bytes=67043328),
            name='attention_block',
        )(hidden, row(seg_ids), w_q, row(b_q), w_kv, row(b_kv), w_o, row(b_o), row(ln_gain), row(ln_bias))

    row_spec = P(('dp', 'cp'), None)
    tok_spec = P(('dp', 'cp'))
    return jax.shard_map(local_block, mesh=mesh,
                         in_specs=(row_spec, tok_spec, P(None, 'tp'), P('tp'), P(None, None), P(None), P('tp', None), P(None), P(None), P(None)),
                         out_specs=(row_spec, row_spec, row_spec), check_vma=False)
```

```python
import functools

import jax
import jax.numpy as jnp
from jax import lax
from jax.experimental import pallas as pl
from jax.experimental.pallas import tpu as pltpu
from jax.sharding import PartitionSpec as P

HEAD_DIM = 128
LN_EPS = 1e-5
SCORE_EXP2 = HEAD_DIM ** -0.5 * 1.4426950408889634
PIECE = 64
Q_COLS = 512
VMEM_LIMIT = 60 * 2 ** 20
SEG_ROWS = 16
MESH_ID = pl.DeviceIdType.MESH
F32 = jnp.float32
BF16 = jnp.bfloat16


def each(lo, hi, body):
    def step(i, carry):
        body(i)
        return carry
    lax.fori_loop(lo, hi, step, 0)


def block_kernel(n_tp, n_cp, hid_hbm, seg_ref, wq_hbm, bq_ref, wkv_hbm, bkv_ref, wo_hbm, bo_ref, gain_ref, lnb_ref,
                 y_v, k_ref, v_ref,
                 normed, gain_f, bias_f, bq_f, bo_f, wkv, wq, wo, kvbuf, segq, q_s, s_buf, m_s, l_s, acc_s, o_s, stage, recv,
                 hid_sem, wkv_sem, wq_sem, wo_sem, kv_send, fwd_send, kv_recv, msg_send, msg_recv,
                 ag_send, ag_recv, fw_send, fw_recv):
    hid = y_v
    tok, d_model = hid.shape
    n_heads = q_s.shape[1] // PIECE
    n_piece = tok // PIECE
    n_chip = n_cp // 2
    chunk = d_model // n_tp
    half = chunk // 2
    q_cols = wq.shape[2]
    n_q = wq.shape[0]
    me_t = lax.axis_index('tp')
    me_c = lax.axis_index('cp')
    chip = me_c // 2
    core = me_c % 2
    sibling = me_c + 1 - 2 * core
    right = (me_t + 1) % n_tp
    left = (me_t + n_tp - 1) % n_tp
    across = (me_t + 2) % n_tp

    ln_rows = tok // 4
    def load_hid(i):
        rows = pl.ds(i * ln_rows, ln_rows)
        return pltpu.make_async_copy(hid_hbm.at[rows, :], hid.at[rows, :], hid_sem.at[i])
    def load_wkv():
        return pltpu.make_async_copy(wkv_hbm, wkv, wkv_sem)
    def load_wq(i):
        return pltpu.make_async_copy(wq_hbm.at[:, pl.ds(i * q_cols, q_cols)], wq.at[i], wq_sem.at[i])
    slots = ((across, 0), (across, 1), (right, 1), (left, 0), (right, 0), (left, 1), (me_t, 0), (me_t, 1))
    def load_wo(i):
        owner, part = slots[i]
        cols = pl.ds(pl.multiple_of(owner * chunk + part * half, 128), half)
        return pltpu.make_async_copy(wo_hbm.at[:, cols], wo.at[i], wo_sem.at[i])
    def wait_wo(i):
        pltpu.make_async_copy(wo_hbm.at[:, pl.ds(0, half)], wo.at[i], wo_sem.at[i]).wait()
    for i in range(4):
        load_hid(i).start()

    barrier = pltpu.get_barrier_semaphore()
    peers = [{'tp': left}, {'tp': right}, {'cp': sibling}] + [{'cp': (me_c + 2 * d) % n_cp} for d in range(1, n_chip)]
    for peer in peers:
        pl.semaphore_signal(barrier, inc=1, device_id=peer, device_id_type=MESH_ID)

    gain_f[...] = gain_ref[...].astype(F32).reshape(gain_f.shape)
    bias_f[...] = lnb_ref[...].astype(F32).reshape(bias_f.shape)
    for i in range(4):
        with jax.named_scope('hid_wait'):
            load_hid(i).wait()
        if i == 0:
            load_wkv().start()
        elif i <= n_q:
            load_wq(i - 1).start()
        with jax.named_scope('norm'):
            rows = slice(i * ln_rows, (i + 1) * ln_rows)
            per_slab = s_buf.shape[1] // ln_rows * (s_buf.shape[2] // HEAD_DIM)
            def kept(b):
                slab, b = divmod(b, per_slab)
                r, c = divmod(b, s_buf.shape[2] // HEAD_DIM)
                return s_buf.at[slab, r * ln_rows:(r + 1) * ln_rows, c * HEAD_DIM:(c + 1) * HEAD_DIM]
            total = jnp.zeros((ln_rows, HEAD_DIM), F32)
            for b in range(d_model // HEAD_DIM):
                x = hid[rows, b * HEAD_DIM:(b + 1) * HEAD_DIM].astype(F32)
                kept(b)[...] = x
                total = total + x
            mean = jnp.broadcast_to(jnp.sum(total, axis=-1, keepdims=True) / d_model, total.shape)
            total = jnp.zeros((ln_rows, HEAD_DIM), F32)
            for b in range(d_model // HEAD_DIM):
                centered = kept(b)[...] - mean
                kept(b)[...] = centered
                total = total + centered * centered
            variance = jnp.sum(total, axis=-1, keepdims=True) / d_model
            scale = jnp.broadcast_to(lax.rsqrt(variance + LN_EPS), total.shape)
            for b in range(d_model // HEAD_DIM):
                cols = slice(b * HEAD_DIM, (b + 1) * HEAD_DIM)
                normed[rows, cols] = (kept(b)[...] * scale * gain_f[:, cols] + bias_f[:, cols]).astype(BF16)
    for i in range(3, n_q):
        load_wq(i).start()

    seg = seg_ref[...]
    seg_high = (seg // 256).astype(F32)
    seg_low = (seg % 256).astype(F32)
    row_id = lax.broadcasted_iota(jnp.int32, (SEG_ROWS, tok), 0)
    kvbuf[me_c, tok:, :] = jnp.where(row_id == 0, seg_high, jnp.where(row_id == 1, seg_low, 0.0)).astype(BF16)
    seg_f = seg.astype(F32)
    for b in range(tok // 128):
        column = jnp.broadcast_to(seg_f[:, b * 128:(b + 1) * 128], (128, 128)).T
        for s in range(128 // PIECE):
            part = column[s * PIECE:(s + 1) * PIECE]
            segq[b * (128 // PIECE) + s] = jnp.concatenate([part] * (tok // 128), axis=1)

    with jax.named_scope('wkv_wait'):
        load_wkv().wait()
    kv = (jnp.dot(normed[...], wkv[...], preferred_element_type=F32) + bkv_ref[...].astype(F32).reshape(1, 2 * HEAD_DIM)).astype(BF16)
    kvbuf[me_c, :tok, :] = kv
    k_ref[...] = kv[:, :HEAD_DIM]
    v_ref[...] = kv[:, HEAD_DIM:]
    with jax.named_scope('barrier_wait'):
        pl.semaphore_wait(barrier, len(peers))

    def send_kv(block, target, send_sem):
        return pltpu.make_async_remote_copy(src_ref=kvbuf.at[block], dst_ref=kvbuf.at[block], send_sem=send_sem,
                                            recv_sem=kv_recv.at[block], device_id={'cp': target}, device_id_type=MESH_ID)
    for d in range(n_chip - 1, 0, -1):
        @pl.when(chip + d < n_chip)
        def _(d=d):
            send_kv(me_c, (me_c + 2 * d) % n_cp, kv_send.at[d]).start()
    @pl.when(core == 0)
    def _():
        send_kv(me_c, sibling, kv_send.at[0]).start()

    bo_f[...] = bo_ref[...].astype(F32).reshape(bo_f.shape)
    bq_f[...] = bq_ref[...].astype(F32).reshape(bq_f.shape)
    for i in range(n_q):
        with jax.named_scope('wq_wait'):
            load_wq(i).wait()
        if i == 0:
            for j in range(8):
                load_wo(j).start()
        q = (jnp.dot(normed[...], wq[i], preferred_element_type=F32) + bq_f[:, i * q_cols:(i + 1) * q_cols]).astype(BF16)
        for piece in range(n_piece):
            for h in range(q_cols // HEAD_DIM):
                head = i * q_cols // HEAD_DIM + h
                q_s[piece, head * PIECE:(head + 1) * PIECE, :] = q[piece * PIECE:(piece + 1) * PIECE, h * HEAD_DIM:(h + 1) * HEAD_DIM]

    def score(piece, blocks, own=None, first=False):
        tops = [] if first else [m_s[...]]
        for block in blocks:
            digits = kvbuf[block, tok:, :].astype(F32)
            visible = segq[piece] == digits[0:1] * 256.0 + digits[1:2]
            if block is own:
                q_pos = lax.broadcasted_iota(jnp.int32, (PIECE, tok), 0) + piece * PIECE
                visible = visible & (lax.broadcasted_iota(jnp.int32, (PIECE, tok), 1) <= q_pos)
            s = lax.dot_general(q_s[piece], kvbuf[block, :tok, :HEAD_DIM], (((1,), (1,)), ((), ())), preferred_element_type=F32)
            s = jnp.where(visible[None], s.reshape(n_heads, PIECE, tok), -jnp.inf).reshape(n_heads * PIECE, tok)
            s_buf[block] = s
            tops += [s[:, b:b + HEAD_DIM] for b in range(0, tok, HEAD_DIM)]
        m_s[...] = functools.reduce(jnp.maximum, tops)

    def weigh(block):
        top = m_s[...]
        parts = [jnp.exp2((s_buf[block, :, b:b + HEAD_DIM] - top) * SCORE_EXP2) for b in range(0, tok, HEAD_DIM)]
        out = jnp.dot(jnp.concatenate(parts, axis=1).astype(BF16), kvbuf[block, :tok, HEAD_DIM:], preferred_element_type=F32)
        return sum(parts), out

    def weigh_pair(i):
        l_first, out_first = weigh(2 * i)
        l_second, out_second = weigh(2 * i + 1)
        l_s[...] += l_first + l_second
        acc_s[...] += out_first + out_second

    def attention_out(piece):
        m_s[...] = jnp.broadcast_to(jnp.max(m_s[...], axis=-1, keepdims=True), m_s.shape)
        @pl.when(core == 0)
        def _():
            l_own, out_own = weigh(me_c)
            l_s[...] = l_own
            acc_s[...] = out_own
        @pl.when(core == 1)
        def _():
            l_s[...] = jnp.zeros_like(l_s)
            acc_s[...] = jnp.zeros_like(acc_s)
        each(0, chip + core, weigh_pair)
        attn = (acc_s[...] / jnp.sum(l_s[...], axis=-1, keepdims=True)).astype(BF16)
        for h in range(n_heads):
            o_s[piece, :, h * HEAD_DIM:(h + 1) * HEAD_DIM] = attn[h * PIECE:(h + 1) * PIECE]

    def score_near(piece):
        @pl.when(core == 0)
        def _():
            score(piece, [me_c], own=me_c, first=True)
        @pl.when(core == 1)
        def _():
            score(piece, [me_c, sibling], own=me_c, first=True)

    def forward(i):
        with jax.named_scope('far_wait_ici'):
            passing = send_kv(me_c - 2 * (i + 1), sibling, fwd_send.at[i])
            passing.wait_recv()
            passing.start()

    def score_far(piece, i, fresh):
        same = me_c - 2 * (i + 1)
        other = sibling - 2 * (i + 1)
        if fresh:
            with jax.named_scope('far_wait_sib'):
                send_kv(other, sibling, fwd_send.at[i]).wait_recv()
        score(piece, [same, other])

    @pl.when(core == 1)
    def _():
        send_kv(sibling, sibling, kv_send.at[0]).wait_recv()
    each(0, jnp.minimum(chip, 2), forward)
    with jax.named_scope('score_near'):
        score_near(0)
    each(jnp.minimum(chip, 2), chip, forward)
    with jax.named_scope('score_far'):
        each(0, chip, lambda i: score_far(0, i, True))

    def message(piece, i):
        target = (me_t + 1 + (i % 2) * (n_tp - 2)) % n_tp
        return pltpu.make_async_remote_copy(src_ref=stage.at[piece, i], dst_ref=recv.at[piece, i], send_sem=msg_send.at[piece, i],
                                            recv_sem=msg_recv.at[piece, i], device_id={'tp': target}, device_id_type=MESH_ID)
    def y_part(piece, owner, part):
        return y_v.at[pl.ds(pl.multiple_of(piece * PIECE, PIECE), PIECE), pl.ds(pl.multiple_of(owner * chunk + part * half, 128), half)]
    def gather(piece, way, part):
        ref = y_part(piece, me_t, part)
        return pltpu.make_async_remote_copy(src_ref=ref, dst_ref=ref, send_sem=ag_send.at[piece, way, part],
                                            recv_sem=ag_recv.at[piece, way, part], device_id={'tp': (right, left)[way]}, device_id_type=MESH_ID)
    def pass_on(piece, way):
        ref = y_part(piece, (left, right)[way], way)
        return pltpu.make_async_remote_copy(src_ref=ref, dst_ref=ref, send_sem=fw_send.at[piece, way],
                                            recv_sem=fw_recv.at[piece, way], device_id={'tp': (right, left)[way]}, device_id_type=MESH_ID)

    def project_first(s):
        def one(i):
            @pl.when(s == 0)
            def _():
                wait_wo(i)
            stage[s, i] = jnp.dot(o_s[s], wo[i], preferred_element_type=F32).astype(BF16)
            message(s, i).start()
        with jax.named_scope('project_first'):
            each(0, 4, one)

    def project_rest(piece, fresh):
        def one(i):
            if fresh is not None:
                @pl.when(fresh)
                def _():
                    wait_wo(i)
            stage[piece, i] = jnp.dot(o_s[piece], wo[i], preferred_element_type=F32).astype(BF16)
            @pl.when(i < 6)
            def _():
                with jax.named_scope('E_wait'):
                    message(piece, i - 4).wait_recv()
                stage[piece, i] = (stage[piece, i].astype(F32) + recv[piece, i - 4].astype(F32)).astype(BF16)
                message(piece, i).start()
        with jax.named_scope('project_rest'):
            each(4, 8, one)

    def add_up(piece):
        with jax.named_scope('G_wait'):
            for i in range(2, 6):
                message(piece, i).wait_recv()
        rows = pl.ds(pl.multiple_of(piece * PIECE, PIECE), PIECE)
        for part in range(2):
            cols = pl.ds(pl.multiple_of(me_t * chunk + part * half, 128), half)
            from_left, from_right = ((4, 3), (2, 5))[part]
            proj = stage[piece, 6 + part].astype(F32) + recv[piece, from_left].astype(F32) + recv[piece, from_right].astype(F32)
            y_v[rows, cols] = (hid[rows, cols].astype(F32) + proj + bo_f[:, cols]).astype(BF16)
            for way in range(2):
                gather(piece, way, part).start()

    def hand_on(piece):
        for way in range(2):
            with jax.named_scope('H_wait'):
                gather(piece, way, way).wait_recv()
            pass_on(piece, way).start()

    def step(s):
        with jax.named_scope('rest_score'):
            @pl.when(s > 0)
            def _():
                score_near(s)
                each(0, chip, lambda i: score_far(s, i, False))
        with jax.named_scope('weigh'):
            attention_out(s)
        project_first(s)
        @pl.when(s == 2)
        def _():
            add_up(0)
        @pl.when(s > 0)
        def _():
            project_rest(s - 1, s == 1)
    each(0, n_piece, step)
    project_rest(n_piece - 1, None)
    each(1, n_piece - 1, add_up)
    hand_on(0)
    add_up(n_piece - 1)
    each(1, n_piece, hand_on)
    with jax.named_scope('I_wait'):
        def arrived(piece):
            for way in range(2):
                gather(piece, way, 1 - way).wait_recv()
                pass_on(piece, way).wait_recv()
        each(0, n_piece, arrived)

    def finish(piece):
        for i in range(6):
            message(piece, i).wait_send()
        for way in range(2):
            for part in range(2):
                gather(piece, way, part).wait_send()
            pass_on(piece, way).wait_send()
    with jax.named_scope('finish'):
        each(0, n_piece, finish)
    for d in range(n_chip - 1, 0, -1):
        @pl.when(chip + d < n_chip)
        def _(d=d):
            send_kv(me_c, (me_c + 2 * d) % n_cp, kv_send.at[d]).wait_send()
    @pl.when(core == 0)
    def _():
        send_kv(me_c, sibling, kv_send.at[0]).wait_send()
    each(0, chip, lambda i: send_kv(me_c - 2 * (i + 1), sibling, fwd_send.at[i]).wait_send())


def store_kernel(*refs):
    copies = [pltpu.make_async_copy(refs[i], refs[3 + i], refs[6].at[i]) for i in range(3)]
    for copy in copies:
        copy.start()
    for copy in copies:
        copy.wait()


def solution(mesh):
    n_tp, n_cp = mesh.shape['tp'], mesh.shape['cp']

    def local_block(hidden, seg_ids, w_q, b_q, w_kv, b_kv, w_o, b_o, ln_gain, ln_bias):
        tok, d_model = hidden.shape
        width = w_q.shape[1]
        n_piece = tok // PIECE
        n_heads = width // HEAD_DIM
        rows = n_heads * PIECE
        half = d_model // n_tp // 2
        hbm = pl.BlockSpec(memory_space=pl.ANY)
        vmem = pl.BlockSpec(memory_space=pltpu.VMEM)
        dma = pltpu.SemaphoreType.DMA
        scratch = [
            pltpu.VMEM((tok, d_model), BF16),
            pltpu.VMEM((1, d_model), F32),
            pltpu.VMEM((1, d_model), F32),
            pltpu.VMEM((1, width), F32),
            pltpu.VMEM((1, d_model), F32),
            pltpu.VMEM((d_model, 2 * HEAD_DIM), BF16),
            pltpu.VMEM((width // Q_COLS, d_model, Q_COLS), BF16),
            pltpu.VMEM((2 * n_tp, width, half), BF16),
            pltpu.VMEM((n_cp, tok + SEG_ROWS, 2 * HEAD_DIM), BF16),
            pltpu.VMEM((n_piece, PIECE, tok), F32),
            pltpu.VMEM((n_piece, rows, HEAD_DIM), BF16),
            pltpu.VMEM((n_cp, rows, tok), F32),
            pltpu.VMEM((rows, HEAD_DIM), F32),
            pltpu.VMEM((rows, HEAD_DIM), F32),
            pltpu.VMEM((rows, HEAD_DIM), F32),
            pltpu.VMEM((n_piece, PIECE, width), BF16),
            pltpu.VMEM((n_piece, 8, PIECE, half), BF16),
            pltpu.VMEM((n_piece, 6, PIECE, half), BF16),
            dma((4,)), dma, dma((width // Q_COLS,)), dma((8,)),
            dma((n_cp // 2,)), dma((n_cp // 2,)), dma((n_cp,)), dma((n_piece, 6)), dma((n_piece, 6)),
            dma((n_piece, 2, 2)), dma((n_piece, 2, 2)), dma((n_piece, 2)), dma((n_piece, 2)),
        ]
        row = lambda a: a.reshape(1, a.shape[0])
        outs = pl.pallas_call(
            functools.partial(block_kernel, n_tp, n_cp),
            out_shape=(pltpu.VMEM((tok, d_model), BF16), pltpu.VMEM((tok, HEAD_DIM), BF16), pltpu.VMEM((tok, HEAD_DIM), BF16)),
            in_specs=[hbm, vmem, hbm, vmem, hbm, vmem, hbm, vmem, vmem, vmem],
            out_specs=(vmem, vmem, vmem),
            scratch_shapes=scratch,
            compiler_params=pltpu.CompilerParams(collective_id=0, has_side_effects=True, vmem_limit_bytes=VMEM_LIMIT),
            name='attention_block',
        )(hidden, row(seg_ids), w_q, b_q, w_kv, b_kv, w_o, b_o, ln_gain, ln_bias)
        return pl.pallas_call(
            store_kernel,
            out_shape=tuple(jax.ShapeDtypeStruct(a.shape, a.dtype) for a in outs),
            in_specs=[vmem] * 3, out_specs=(hbm,) * 3,
            scratch_shapes=[dma((3,))],
            compiler_params=pltpu.CompilerParams(vmem_limit_bytes=2 ** 20),
            name='store_outputs',
        )(*[pltpu.with_memory_space_constraint(a, pltpu.VMEM) for a in outs])

    row_spec = P(('dp', 'cp'), None)
    tok_spec = P(('dp', 'cp'))
    return jax.shard_map(local_block, mesh=mesh,
                         in_specs=(row_spec, tok_spec, P(None, 'tp'), P('tp'), P(None, None), P(None), P('tp', None), P(None), P(None), P(None)),
                         out_specs=(row_spec, row_spec, row_spec), check_vma=False)
```

```python
import functools

import jax
import jax.numpy as jnp
from jax import lax
from jax.experimental import pallas as pl
from jax.experimental.pallas import tpu as pltpu
from jax.sharding import PartitionSpec as P

HEAD_DIM = 128
LN_EPS = 1e-5
SCORE_EXP2 = HEAD_DIM ** -0.5 * 1.4426950408889634
PIECE = 64
Q_COLS = 512
SCORE_HEADS = 6
WEIGH_HEADS = 6
VMEM_LIMIT = 60 * 2 ** 20
SEG_ROWS = 16
MESH_ID = pl.DeviceIdType.MESH
F32 = jnp.float32
BF16 = jnp.bfloat16


def each(lo, hi, body):
    def step(i, carry):
        body(i)
        return carry
    lax.fori_loop(lo, hi, step, 0)


def block_kernel(n_tp, n_cp, hid_hbm, seg_hbm, wq_hbm, bq_hbm, wkv_hbm, bkv_hbm, wo_hbm, bo_hbm, gain_hbm, lnb_hbm,
                 y_v, k_ref, v_ref,
                 seg_ref, bq_ref, bkv_ref, bo_ref, gain_ref, lnb_ref, normed, gain_f, bias_f, bq_f, bo_f, wkv, wq, wo, kvbuf, segq, q_s, s_buf, m_s, l_s, acc_s, o_s, stage, recv,
                 small_sem, hid_sem, wkv_sem, wq_sem, wo_sem, kv_send, fwd_send, kv_recv, msg_send, msg_recv,
                 ag_send, ag_recv, fw_send, fw_recv):
    hid = y_v
    tok, d_model = hid.shape
    n_heads = q_s.shape[1] // PIECE
    n_piece = tok // PIECE
    n_chip = n_cp // 2
    chunk = d_model // n_tp
    half = chunk // 2
    q_cols = wq.shape[2]
    n_q = wq.shape[0]
    me_t = lax.axis_index('tp')
    me_c = lax.axis_index('cp')
    chip = me_c // 2
    core = me_c % 2
    sibling = me_c + 1 - 2 * core
    right = (me_t + 1) % n_tp
    left = (me_t + n_tp - 1) % n_tp
    across = (me_t + 2) % n_tp

    ln_rows = tok // 4
    def load_hid(i):
        parts = [(i + 3, i * ln_rows, ln_rows)] if i else [(j, j * ln_rows // 4, ln_rows // 4) for j in range(4)]
        return [pltpu.make_async_copy(hid_hbm.at[pl.ds(at, n), :], hid.at[pl.ds(at, n), :], hid_sem.at[j]) for j, at, n in parts]
    small = [pltpu.make_async_copy(src, dst, small_sem.at[i]) for i, (src, dst) in enumerate((
        (gain_hbm, gain_ref), (lnb_hbm, lnb_ref), (seg_hbm, seg_ref), (bkv_hbm, bkv_ref), (bq_hbm, bq_ref), (bo_hbm, bo_ref)))]
    def load_wkv():
        return pltpu.make_async_copy(wkv_hbm, wkv, wkv_sem)
    def load_wq(i):
        return pltpu.make_async_copy(wq_hbm.at[:, pl.ds(i * q_cols, q_cols)], wq.at[i], wq_sem.at[i])
    slots = ((across, 0), (across, 1), (right, 1), (left, 0), (right, 0), (left, 1), (me_t, 0), (me_t, 1))
    def load_wo(i):
        owner, part = slots[i]
        cols = pl.ds(pl.multiple_of(owner * chunk + part * half, 128), half)
        return pltpu.make_async_copy(wo_hbm.at[:, cols], wo.at[i], wo_sem.at[i])
    def wait_wo(i):
        pltpu.make_async_copy(wo_hbm.at[:, pl.ds(0, half)], wo.at[i], wo_sem.at[i]).wait()
    for i in range(4):
        for copy in load_hid(i):
            copy.start()
        if i == 0:
            for copy in small:
                copy.start()

    barrier = pltpu.get_barrier_semaphore()
    peers = [{'tp': left}, {'tp': right}, {'cp': sibling}] + [{'cp': (me_c + 2 * d) % n_cp} for d in range(1, n_chip)]
    for peer in peers:
        pl.semaphore_signal(barrier, inc=1, device_id=peer, device_id_type=MESH_ID)

    def norm_rows(i):
        rows = slice(i * ln_rows, (i + 1) * ln_rows)
        per_slab = s_buf.shape[1] // ln_rows * (s_buf.shape[2] // HEAD_DIM)
        n_col = d_model // HEAD_DIM
        def kept(b):
            slab, b = divmod(b + i * n_col, per_slab)
            r, c = divmod(b, s_buf.shape[2] // HEAD_DIM)
            return s_buf.at[slab, r * ln_rows:(r + 1) * ln_rows, c * HEAD_DIM:(c + 1) * HEAD_DIM]
        total = jnp.zeros((ln_rows, HEAD_DIM), F32)
        for b in range(n_col):
            x = hid[rows, b * HEAD_DIM:(b + 1) * HEAD_DIM].astype(F32)
            kept(b)[...] = x
            total = total + x
        mean = jnp.broadcast_to(jnp.sum(total, axis=-1, keepdims=True) / d_model, total.shape)
        total = jnp.zeros((ln_rows, HEAD_DIM), F32)
        for b in range(n_col):
            centered = kept(b)[...] - mean
            kept(b)[...] = centered
            total = total + centered * centered
        variance = jnp.sum(total, axis=-1, keepdims=True) / d_model
        scale = jnp.broadcast_to(lax.rsqrt(variance + LN_EPS), total.shape)
        if i == 0:
            for copy in small:
                copy.wait()
            gain_f[...] = gain_ref[...].astype(F32).reshape(gain_f.shape)
            bias_f[...] = lnb_ref[...].astype(F32).reshape(bias_f.shape)
        for b in range(n_col):
            cols = slice(b * HEAD_DIM, (b + 1) * HEAD_DIM)
            normed[rows, cols] = (kept(b)[...] * scale * gain_f[:, cols] + bias_f[:, cols]).astype(BF16)

    with jax.named_scope('hid_wait'):
        for copy in load_hid(0):
            copy.wait()
    load_wkv().start()
    load_wq(0).start()
    with jax.named_scope('norm'):
        norm_rows(0)
    with jax.named_scope('hid_wait'):
        for i in range(1, 4):
            for copy in load_hid(i):
                copy.wait()
    with jax.named_scope('norm'):
        for i in range(1, 4):
            norm_rows(i)
    for i in range(1, n_q):
        load_wq(i).start()

    seg = seg_ref[...]
    seg_high = (seg // 256).astype(F32)
    seg_low = (seg % 256).astype(F32)
    row_id = lax.broadcasted_iota(jnp.int32, (SEG_ROWS, tok), 0)
    kvbuf[me_c, tok:, :] = jnp.where(row_id == 0, seg_high, jnp.where(row_id == 1, seg_low, 0.0)).astype(BF16)
    seg_f = seg.astype(F32)
    for b in range(tok // 128):
        column = jnp.broadcast_to(seg_f[:, b * 128:(b + 1) * 128], (128, 128)).T
        for s in range(128 // PIECE):
            part = column[s * PIECE:(s + 1) * PIECE]
            segq[b * (128 // PIECE) + s] = jnp.concatenate([part] * (tok // 128), axis=1)

    with jax.named_scope('wkv_wait'):
        load_wkv().wait()
    kv = (jnp.dot(normed[...], wkv[...], preferred_element_type=F32) + bkv_ref[...].astype(F32).reshape(1, 2 * HEAD_DIM)).astype(BF16)
    kvbuf[me_c, :tok, :] = kv
    k_ref[...] = kv[:, :HEAD_DIM]
    v_ref[...] = kv[:, HEAD_DIM:]
    with jax.named_scope('barrier_wait'):
        pl.semaphore_wait(barrier, len(peers))

    def send_kv(block, target, send_sem):
        return pltpu.make_async_remote_copy(src_ref=kvbuf.at[block], dst_ref=kvbuf.at[block], send_sem=send_sem,
                                            recv_sem=kv_recv.at[block], device_id={'cp': target}, device_id_type=MESH_ID)
    for d in range(n_chip - 1, 0, -1):
        @pl.when(chip + d < n_chip)
        def _(d=d):
            send_kv(me_c, (me_c + 2 * d) % n_cp, kv_send.at[d]).start()
    @pl.when(core == 0)
    def _():
        send_kv(me_c, sibling, kv_send.at[0]).start()

    def forward(i):
        with jax.named_scope('far_wait_ici'):
            passing = send_kv(me_c - 2 * (i + 1), sibling, fwd_send.at[i])
            passing.wait_recv()
            passing.start()

    bo_f[...] = bo_ref[...].astype(F32).reshape(bo_f.shape)
    bq_f[...] = bq_ref[...].astype(F32).reshape(bq_f.shape)
    for i in range(n_q):
        with jax.named_scope('wq_wait'):
            load_wq(i).wait()
        if i == 0:
            for j in range(8):
                load_wo(j).start()
        q = (jnp.dot(normed[...], wq[i], preferred_element_type=F32) + bq_f[:, i * q_cols:(i + 1) * q_cols]).astype(BF16)
        for piece in range(n_piece):
            for h in range(q_cols // HEAD_DIM):
                head = i * q_cols // HEAD_DIM + h
                q_s[piece, head * PIECE:(head + 1) * PIECE, :] = q[piece * PIECE:(piece + 1) * PIECE, h * HEAD_DIM:(h + 1) * HEAD_DIM]

    def score(piece, blocks, own=None, first=False):
        hides = []
        for block in blocks:
            digits = kvbuf[block, tok:, :].astype(F32)
            visible = segq[piece] == digits[0:1] * 256.0 + digits[1:2]
            if block is own:
                q_pos = lax.broadcasted_iota(jnp.int32, (PIECE, tok), 0) + piece * PIECE
                visible = visible & (lax.broadcasted_iota(jnp.int32, (PIECE, tok), 1) <= q_pos)
            hides.append(visible[None])
        for r in range(0, n_heads, SCORE_HEADS):
            rows = slice(r * PIECE, (r + SCORE_HEADS) * PIECE)
            tops = [] if first else [m_s[rows]]
            for block, visible in zip(blocks, hides):
                s = lax.dot_general(q_s[piece, rows], kvbuf[block, :tok, :HEAD_DIM], (((1,), (1,)), ((), ())), preferred_element_type=F32)
                s = jnp.where(visible, (s * SCORE_EXP2).reshape(SCORE_HEADS, PIECE, tok), -jnp.inf).reshape(SCORE_HEADS * PIECE, tok)
                s_buf[block, rows] = s
                tops += [s[:, b:b + HEAD_DIM] for b in range(0, tok, HEAD_DIM)]
            m_s[rows] = functools.reduce(jnp.maximum, tops)

    def weigh_some(blocks):
        v_all = jnp.concatenate([kvbuf[block, :tok, HEAD_DIM:] for block in blocks], axis=0)
        for r in range(0, n_heads, WEIGH_HEADS):
            rows = slice(r * PIECE, (r + WEIGH_HEADS) * PIECE)
            top = m_s[rows]
            parts = [jnp.exp2(s_buf[block, rows, b:b + HEAD_DIM] - top) for block in blocks for b in range(0, tok, HEAD_DIM)]
            l_s[rows] += sum(parts)
            acc_s[rows] += jnp.dot(jnp.concatenate(parts, axis=1).astype(BF16), v_all, preferred_element_type=F32)

    def attention_out(piece):
        m_s[...] = jnp.broadcast_to(jnp.max(m_s[...], axis=-1, keepdims=True), m_s.shape)
        l_s[...] = jnp.zeros_like(l_s)
        acc_s[...] = jnp.zeros_like(acc_s)
        n_block = me_c + 1
        each(0, n_block // 4, lambda i: weigh_some([4 * i + j for j in range(4)]))
        @pl.when(n_block % 4 >= 2)
        def _():
            at = n_block // 4 * 4
            weigh_some([at, at + 1])
        @pl.when(n_block % 2 == 1)
        def _():
            weigh_some([me_c])
        attn = (acc_s[...] / jnp.sum(l_s[...], axis=-1, keepdims=True)).astype(BF16)
        for h in range(n_heads):
            o_s[piece, :, h * HEAD_DIM:(h + 1) * HEAD_DIM] = attn[h * PIECE:(h + 1) * PIECE]

    def score_near(piece):
        @pl.when(core == 0)
        def _():
            score(piece, [me_c], own=me_c, first=True)
        @pl.when(core == 1)
        def _():
            score(piece, [me_c, sibling], own=me_c, first=True)

    def far(i):
        return me_c - 2 * (i + 1), sibling - 2 * (i + 1)

    def wait_passed(i):
        with jax.named_scope('far_wait_sib'):
            send_kv(far(i)[1], sibling, fwd_send.at[i]).wait_recv()

    @pl.when(core == 1)
    def _():
        send_kv(sibling, sibling, kv_send.at[0]).wait_recv()
    each(0, jnp.minimum(chip, 2), forward)
    with jax.named_scope('score_near'):
        score_near(0)
    each(jnp.minimum(chip, 2), chip, forward)
    with jax.named_scope('score_far'):
        def listed(j):
            here = j < chip
            @pl.when(j >= chip)
            def _():
                wait_passed(j - chip)
            return jnp.where(here, me_c - 2 * (j + 1), sibling - 2 * (j - chip + 1))
        each(0, chip, lambda i: score(0, [listed(2 * i), listed(2 * i + 1)]))

    def message(piece, i):
        target = (me_t + 1 + (i % 2) * (n_tp - 2)) % n_tp
        return pltpu.make_async_remote_copy(src_ref=stage.at[piece, i], dst_ref=recv.at[piece, i], send_sem=msg_send.at[piece, i],
                                            recv_sem=msg_recv.at[piece, i], device_id={'tp': target}, device_id_type=MESH_ID)
    def y_part(piece, owner, part):
        return y_v.at[pl.ds(pl.multiple_of(piece * PIECE, PIECE), PIECE), pl.ds(pl.multiple_of(owner * chunk + part * half, 128), half)]
    def gather(piece, way, part):
        ref = y_part(piece, me_t, part)
        return pltpu.make_async_remote_copy(src_ref=ref, dst_ref=ref, send_sem=ag_send.at[piece, way, part],
                                            recv_sem=ag_recv.at[piece, way, part], device_id={'tp': (right, left)[way]}, device_id_type=MESH_ID)
    def pass_on(piece, way):
        ref = y_part(piece, (left, right)[way], way)
        return pltpu.make_async_remote_copy(src_ref=ref, dst_ref=ref, send_sem=fw_send.at[piece, way],
                                            recv_sem=fw_recv.at[piece, way], device_id={'tp': (right, left)[way]}, device_id_type=MESH_ID)

    def project(piece):
        def one(j):
            i = j + 2 * (j // 2 % 2) - 2 * (j // 4)
            @pl.when(piece == 0)
            def _():
                wait_wo(i)
            stage[piece, i] = jnp.dot(o_s[piece], wo[i], preferred_element_type=F32).astype(BF16)
            @pl.when(i < 4)
            def _():
                message(piece, i).start()
        with jax.named_scope('project'):
            each(0, 6, one)

    def relay(piece):
        for i in range(2):
            with jax.named_scope('E_wait'):
                message(piece, i).wait_recv()
            stage[piece, 4 + i] = (stage[piece, 4 + i].astype(F32) + recv[piece, i].astype(F32)).astype(BF16)
            message(piece, 4 + i).start()

    def project_own(piece, fresh=None):
        def one(i):
            if fresh is not None:
                @pl.when(fresh)
                def _():
                    wait_wo(i)
            stage[piece, i] = jnp.dot(o_s[piece], wo[i], preferred_element_type=F32).astype(BF16)
        with jax.named_scope('project_own'):
            each(6, 8, one)

    def add_up(piece):
        with jax.named_scope('G_wait'):
            for i in range(2, 6):
                message(piece, i).wait_recv()
        rows = pl.ds(pl.multiple_of(piece * PIECE, PIECE), PIECE)
        for part in range(2):
            cols = pl.ds(pl.multiple_of(me_t * chunk + part * half, 128), half)
            from_left, from_right = ((4, 3), (2, 5))[part]
            proj = stage[piece, 6 + part].astype(F32) + recv[piece, from_left].astype(F32) + recv[piece, from_right].astype(F32)
            y_v[rows, cols] = (hid[rows, cols].astype(F32) + proj + bo_f[:, cols]).astype(BF16)
            for way in range(2):
                gather(piece, way, part).start()

    def hand_on(piece):
        for way in range(2):
            with jax.named_scope('H_wait'):
                gather(piece, way, way).wait_recv()
            pass_on(piece, way).start()

    def step(s):
        @pl.when(s > 0)
        def _():
            with jax.named_scope('rest_score'):
                score_near(s)
                each(0, chip, lambda i: score(s, far(i)))
            relay(s - 1)
        with jax.named_scope('weigh'):
            attention_out(s)
        project(s)
        @pl.when(s > 0)
        def _():
            project_own(s - 1, s == 1)
        @pl.when((s > 0) & (s < n_piece - 1))
        def _():
            add_up(s - 1)
    each(0, n_piece, step)
    last = n_piece - 1
    hand_on(0)
    project_own(last)
    relay(last)
    add_up(last - 1)
    add_up(last)
    with jax.named_scope('send_wait'):
        for way in range(2):
            gather(last, way, 0).wait_send()
    hand_on(1)
    with jax.named_scope('send_wait'):
        for way in range(2):
            gather(last, way, 1).wait_send()
    each(2, n_piece, hand_on)
    with jax.named_scope('I_wait'):
        def arrived(piece):
            for way in range(2):
                gather(piece, way, 1 - way).wait_recv()
                pass_on(piece, way).wait_recv()
        each(0, n_piece, arrived)

    def finish(piece):
        for i in range(6):
            message(piece, i).wait_send()
        for way in range(2):
            @pl.when(piece < last)
            def _():
                for part in range(2):
                    gather(piece, way, part).wait_send()
            pass_on(piece, way).wait_send()
    with jax.named_scope('finish'):
        each(0, n_piece, finish)
    for d in range(n_chip - 1, 0, -1):
        @pl.when(chip + d < n_chip)
        def _(d=d):
            send_kv(me_c, (me_c + 2 * d) % n_cp, kv_send.at[d]).wait_send()
    @pl.when(core == 0)
    def _():
        send_kv(me_c, sibling, kv_send.at[0]).wait_send()
    each(0, chip, lambda i: send_kv(me_c - 2 * (i + 1), sibling, fwd_send.at[i]).wait_send())


def store_kernel(*refs):
    y_v, k_v, v_v, y_out, k_out, v_out, sem = refs
    rows = y_v.shape[0] // 4
    parts = [(y_v.at[pl.ds(i * rows, rows), :], y_out.at[pl.ds(i * rows, rows), :]) for i in range(4)]
    copies = [pltpu.make_async_copy(src, dst, sem.at[i]) for i, (src, dst) in enumerate(parts + [(k_v, k_out), (v_v, v_out)])]
    for copy in copies:
        copy.start()
    for copy in copies:
        copy.wait()


def solution(mesh):
    n_tp, n_cp = mesh.shape['tp'], mesh.shape['cp']

    def local_block(hidden, seg_ids, w_q, b_q, w_kv, b_kv, w_o, b_o, ln_gain, ln_bias):
        tok, d_model = hidden.shape
        width = w_q.shape[1]
        n_piece = tok // PIECE
        n_heads = width // HEAD_DIM
        rows = n_heads * PIECE
        half = d_model // n_tp // 2
        hbm = pl.BlockSpec(memory_space=pl.ANY)
        vmem = pl.BlockSpec(memory_space=pltpu.VMEM)
        dma = pltpu.SemaphoreType.DMA
        scratch = [
            pltpu.VMEM((1, tok), jnp.int32),
            pltpu.VMEM(b_q.shape, BF16), pltpu.VMEM(b_kv.shape, BF16), pltpu.VMEM(b_o.shape, BF16),
            pltpu.VMEM(ln_gain.shape, BF16), pltpu.VMEM(ln_bias.shape, BF16),
            pltpu.VMEM((tok, d_model), BF16),
            pltpu.VMEM((1, d_model), F32),
            pltpu.VMEM((1, d_model), F32),
            pltpu.VMEM((1, width), F32),
            pltpu.VMEM((1, d_model), F32),
            pltpu.VMEM((d_model, 2 * HEAD_DIM), BF16),
            pltpu.VMEM((width // Q_COLS, d_model, Q_COLS), BF16),
            pltpu.VMEM((2 * n_tp, width, half), BF16),
            pltpu.VMEM((n_cp, tok + SEG_ROWS, 2 * HEAD_DIM), BF16),
            pltpu.VMEM((n_piece, PIECE, tok), F32),
            pltpu.VMEM((n_piece, rows, HEAD_DIM), BF16),
            pltpu.VMEM((n_cp, rows, tok), F32),
            pltpu.VMEM((rows, HEAD_DIM), F32),
            pltpu.VMEM((rows, HEAD_DIM), F32),
            pltpu.VMEM((rows, HEAD_DIM), F32),
            pltpu.VMEM((n_piece, PIECE, width), BF16),
            pltpu.VMEM((n_piece, 8, PIECE, half), BF16),
            pltpu.VMEM((n_piece, 6, PIECE, half), BF16),
            dma((6,)), dma((7,)), dma, dma((width // Q_COLS,)), dma((8,)),
            dma((n_cp // 2,)), dma((n_cp // 2,)), dma((n_cp,)), dma((n_piece, 6)), dma((n_piece, 6)),
            dma((n_piece, 2, 2)), dma((n_piece, 2, 2)), dma((n_piece, 2)), dma((n_piece, 2)),
        ]
        row = lambda a: a.reshape(1, a.shape[0])
        outs = pl.pallas_call(
            functools.partial(block_kernel, n_tp, n_cp),
            out_shape=(pltpu.VMEM((tok, d_model), BF16), pltpu.VMEM((tok, HEAD_DIM), BF16), pltpu.VMEM((tok, HEAD_DIM), BF16)),
            in_specs=[hbm] * 10,
            out_specs=(vmem, vmem, vmem),
            scratch_shapes=scratch,
            compiler_params=pltpu.CompilerParams(collective_id=0, has_side_effects=True, vmem_limit_bytes=VMEM_LIMIT),
            name='attention_block',
        )(hidden, row(seg_ids), w_q, b_q, w_kv, b_kv, w_o, b_o, ln_gain, ln_bias)
        return pl.pallas_call(
            store_kernel,
            out_shape=tuple(jax.ShapeDtypeStruct(a.shape, a.dtype) for a in outs),
            in_specs=[vmem] * 3, out_specs=(hbm,) * 3,
            scratch_shapes=[dma((6,))],
            compiler_params=pltpu.CompilerParams(vmem_limit_bytes=2 ** 20),
            name='store_outputs',
        )(*[pltpu.with_memory_space_constraint(a, pltpu.VMEM) for a in outs])

    row_spec = P(('dp', 'cp'), None)
    tok_spec = P(('dp', 'cp'))
    return jax.shard_map(local_block, mesh=mesh,
                         in_specs=(row_spec, tok_spec, P(None, 'tp'), P('tp'), P(None, None), P(None), P('tp', None), P(None), P(None), P(None)),
                         out_specs=(row_spec, row_spec, row_spec), check_vma=False)
```
